32 devices in a mesh: rep: 1 (over z), tp: 4 (over y), sp: 8 (over x, core).
Axes of the slice: x: 4, y: 4, z: 1, core: 2. Of those that a mesh axis runs over, the one named last changes fastest.
The devices are a block of a 4x4x8 slice.
Arguments:
- x_tokens: bfloat16 [6144, 5120], P(('rep', 'sp'))
- positions: int32 [6144], P(('rep', 'sp'))
- gains: float32 [2, 4, 5120], replicated
- w_q: bfloat16 [2, 5120, 32, 128], P(None, None, 'tp')
- w_k: bfloat16 [2, 5120, 8, 128], P(None, None, 'tp')
- w_v: bfloat16 [2, 5120, 8, 128], P(None, None, 'tp')
- w_o: bfloat16 [2, 32, 128, 5120], P(None, 'tp')
- w_gate: bfloat16 [2, 5120, 14336], P(None, None, 'tp')
- w_up: bfloat16 [2, 5120, 14336], P(None, None, 'tp')
- w_down: bfloat16 [2, 14336, 5120], P(None, 'tp')
Outputs:
- output 1: bfloat16 [6144, 5120], P(('rep', 'sp'))
- output 2: bfloat16 [512, 32, 128], P('rep', ('tp', 'sp'))
- output 3: bfloat16 [512, 32, 128], P('rep', ('tp', 'sp'))
- output 4: bfloat16 [6144, 32, 128], P('rep', ('tp', 'sp'))
- output 5: bfloat16 [6144, 32, 128], P('rep', ('tp', 'sp'))
All inputs are finite; a program needn't handle non-finite values.
Results may differ from the reference program's by a relative error of at most 0.0162716.
Values are sent between devices in bfloat16 or wider.
A program may use at most 768 MiB of HBM per device.

```python
import jax
import jax.numpy as jnp
from jax import lax

D = 5120
HEADS = 32
KV_HEADS = 8
HEAD = 128
FF = 14336
TOKENS = 6144
WINDOW = 512
CACHE_HEADS = 32
REF_BLOCK = 64

GROUP_SIZE = HEADS // KV_HEADS
REPEAT = CACHE_HEADS // KV_HEADS
NORM_EPS = 1e-6
LOCAL_BASE = 10000.0
GLOBAL_BASE = 1000000.0


def setup_inputs(seed: int = 0, part: int = 0) -> dict:
    part_key = jax.random.fold_in(jax.random.key(seed), part)
    key_x, key_pos = jax.random.split(part_key, 2)
    weight_keys = jax.random.split(jax.random.key(seed + 1), 8)
    x_tokens = jax.random.normal(key_x, (TOKENS, D), jnp.float32).astype(jnp.bfloat16)
    start = jax.random.randint(key_pos, (), 0, 4096)
    positions = (start + jnp.arange(TOKENS)).astype(jnp.int32)
    gains = 1.0 + 0.25 * jax.random.normal(weight_keys[0], (2, 4, D), jnp.float32)

    def weight(key, shape, fan_in):
        return (jax.random.normal(key, shape, jnp.float32) * fan_in ** -0.5).astype(jnp.bfloat16)

    return {
        'x_tokens': x_tokens,
        'positions': positions,
        'gains': gains,
        'w_q': weight(weight_keys[1], (2, D, HEADS, HEAD), D),
        'w_k': weight(weight_keys[2], (2, D, KV_HEADS, HEAD), D),
        'w_v': weight(weight_keys[3], (2, D, KV_HEADS, HEAD), D),
        'w_o': weight(weight_keys[4], (2, HEADS, HEAD, D), HEADS * HEAD),
        'w_gate': weight(weight_keys[5], (2, D, FF), D),
        'w_up': weight(weight_keys[6], (2, D, FF), D),
        'w_down': weight(weight_keys[7], (2, FF, D), FF),
    }


def rms_norm(values, gain):
    wide = values.astype(jnp.float32)
    inv_rms = lax.rsqrt(jnp.mean(wide * wide, axis=-1, keepdims=True) + NORM_EPS)
    return wide * inv_rms * gain


def rotary(projected, positions, base):
    half = projected.shape[-1] // 2
    inv_freq = base ** (-jnp.arange(half, dtype=jnp.float32) / half)
    angles = positions.astype(jnp.float32)[..., None] * inv_freq
    cos_part = jnp.cos(angles)[..., None, :]
    sin_part = jnp.sin(angles)[..., None, :]
    first = projected[..., :half]
    second = projected[..., half:]
    return jnp.concatenate([first * cos_part - second * sin_part, second * cos_part + first * sin_part], axis=-1)


def attention(q_rot, k_rot, v_new, local):
    q_wide = q_rot.reshape(TOKENS, KV_HEADS, GROUP_SIZE, HEAD).astype(jnp.float32)
    k_wide = k_rot.astype(jnp.float32)
    v_wide = v_new.astype(jnp.float32)
    span = WINDOW + REF_BLOCK if local else TOKENS

    def one_block(block_id):
        q_start = block_id * REF_BLOCK
        q_tile = lax.dynamic_slice_in_dim(q_wide, q_start, REF_BLOCK, 0)
        q_idx = q_start + jnp.arange(REF_BLOCK)
        k_start = jnp.clip(q_start - WINDOW, 0, TOKENS - span) if local else 0
        k_tile = lax.dynamic_slice_in_dim(k_wide, k_start, span, 0)
        v_tile = lax.dynamic_slice_in_dim(v_wide, k_start, span, 0)
        k_idx = k_start + jnp.arange(span)
        allowed = k_idx[None, :] <= q_idx[:, None]
        if local:
            allowed = allowed & (q_idx[:, None] - k_idx[None, :] < WINDOW)
        scores = jnp.einsum('qhgd,khd->hgqk', q_tile, k_tile) * (HEAD ** -0.5)
        weights = jax.nn.softmax(jnp.where(allowed, scores, -1e30), axis=-1)
        weights = weights.astype(jnp.bfloat16).astype(jnp.float32)
        return jnp.einsum('hgqk,khd->qhgd', weights, v_tile).astype(jnp.bfloat16)

    blocks = lax.map(one_block, jnp.arange(TOKENS // REF_BLOCK))
    return blocks.reshape(TOKENS, HEADS * HEAD)


def layer(hidden, positions, gain, w_q, w_k, w_v, w_o, w_gate, w_up, w_down, local):
    base = LOCAL_BASE if local else GLOBAL_BASE
    u_norm = rms_norm(hidden, gain[0]).astype(jnp.bfloat16)
    q_proj = jnp.dot(u_norm, w_q.reshape(D, HEADS * HEAD), preferred_element_type=jnp.float32)
    k_proj = jnp.dot(u_norm, w_k.reshape(D, KV_HEADS * HEAD), preferred_element_type=jnp.float32)
    v_proj = jnp.dot(u_norm, w_v.reshape(D, KV_HEADS * HEAD), preferred_element_type=jnp.float32)
    q_rot = rotary(q_proj.reshape(TOKENS, HEADS, HEAD), positions, base).astype(jnp.bfloat16)
    k_rot = rotary(k_proj.reshape(TOKENS, KV_HEADS, HEAD), positions, base).astype(jnp.bfloat16)
    v_new = v_proj.reshape(TOKENS, KV_HEADS, HEAD).astype(jnp.bfloat16)
    attn_out = attention(q_rot, k_rot, v_new, local)
    o_sum = jnp.dot(attn_out, w_o.reshape(HEADS * HEAD, D), preferred_element_type=jnp.float32)
    x_mid = (hidden.astype(jnp.float32) + rms_norm(o_sum, gain[1])).astype(jnp.bfloat16)
    u_mlp = rms_norm(x_mid, gain[2]).astype(jnp.bfloat16)
    gate_pre = jnp.dot(u_mlp, w_gate, preferred_element_type=jnp.float32)
    up_pre = jnp.dot(u_mlp, w_up, preferred_element_type=jnp.float32)
    hidden_act = (jax.nn.silu(gate_pre) * up_pre).astype(jnp.bfloat16)
    m_sum = jnp.dot(hidden_act, w_down, preferred_element_type=jnp.float32)
    x_out = (x_mid.astype(jnp.float32) + rms_norm(m_sum, gain[3])).astype(jnp.bfloat16)
    k_cache = jnp.repeat(k_rot, REPEAT, axis=1)
    v_cache = jnp.repeat(v_new, REPEAT, axis=1)
    if local:
        return x_out, k_cache[TOKENS - WINDOW:], v_cache[TOKENS - WINDOW:]
    return x_out, k_cache, v_cache


def reference(x_tokens, positions, gains, w_q, w_k, w_v, w_o, w_gate, w_up, w_down):
    hidden, k_local, v_local = layer(x_tokens, positions, gains[0], w_q[0], w_k[0], w_v[0], w_o[0], w_gate[0], w_up[0], w_down[0], True)
    out_hidden, k_global, v_global = layer(hidden, positions, gains[1], w_q[1], w_k[1], w_v[1], w_o[1], w_gate[1], w_up[1], w_down[1], False)
    return out_hidden, k_local, v_local, k_global, v_global
```

```python
import functools
import math

import jax
import jax.numpy as jnp
from jax import lax
from jax.experimental import pallas as pl
from jax.experimental.pallas import tpu as pltpu
from jax.sharding import PartitionSpec as P


NORM_EPS = 1e-6
WINDOW = 512
Q_BLOCK = 256
LOCAL_BASE = 10000.0
GLOBAL_BASE = 1000000.0
CHUNKS = 2
F32 = jnp.float32
BF16 = jnp.bfloat16
NEG = -1e30


def rms_norm(values, gain):
    wide = values.astype(F32)
    inv_rms = lax.rsqrt(jnp.mean(wide * wide, axis=-1, keepdims=True) + NORM_EPS)
    return wide * inv_rms * gain


def rope_tables(positions, half, base):
    inv_freq = base ** (-jnp.arange(half, dtype=F32) / half)
    angles = positions.astype(F32)[:, None] * inv_freq
    cos, sin = jnp.cos(angles), jnp.sin(angles)
    return jnp.concatenate([cos, cos], axis=1), jnp.concatenate([-sin, sin], axis=1)


def rotate(x, cos, sin):
    return (x * cos + pltpu.roll(x, x.shape[-1] // 2, 1) * sin).astype(BF16)


def rope_local_kernel(q_ref, k_ref, v_ref, cos_ref, sin_ref, qo_ref, ko_ref, vo_ref):
    head_dim = cos_ref.shape[1]
    cos, sin = cos_ref[...], sin_ref[...]
    for h in range(qo_ref.shape[0]):
        qo_ref[h] = rotate(q_ref[:, h * head_dim:(h + 1) * head_dim], cos, sin)
    for h in range(ko_ref.shape[0]):
        ko_ref[h] = rotate(k_ref[:, h * head_dim:(h + 1) * head_dim], cos, sin)
        vo_ref[h] = v_ref[:, h * head_dim:(h + 1) * head_dim].astype(BF16)


def rope_local(q, k, v, cos, sin):
    tokens, head_dim = cos.shape
    n_q, n_k = q.shape[1] // head_dim, k.shape[1] // head_dim
    return pl.pallas_call(
        rope_local_kernel,
        out_shape=[jax.ShapeDtypeStruct((n, tokens, head_dim), BF16) for n in (n_q, n_k, n_k)],
        cost_estimate=pl.CostEstimate(flops=4 * q.size, bytes_accessed=8 * q.size, transcendentals=0),
        name='rope_local',
    )(q, k, v, cos, sin)


def rope_send_kernel(repeat, q_ref, k_ref, v_ref, cos_ref, sin_ref, out_ref):
    head_dim = cos_ref.shape[1]
    cos, sin = cos_ref[...], sin_ref[...]
    n_q = out_ref.shape[0]
    for h in range(n_q):
        out_ref[h, 0] = rotate(q_ref[:, h * head_dim:(h + 1) * head_dim], cos, sin)
    for g in range(n_q // repeat):
        k = rotate(k_ref[:, g * head_dim:(g + 1) * head_dim], cos, sin)
        v = v_ref[:, g * head_dim:(g + 1) * head_dim].astype(BF16)
        for h in range(g * repeat, (g + 1) * repeat):
            out_ref[h, 1] = k
            out_ref[h, 2] = v


def rope_send(q, k, v, cos, sin):
    tokens, head_dim = cos.shape
    n_q, n_k = q.shape[1] // head_dim, k.shape[1] // head_dim
    return pl.pallas_call(
        functools.partial(rope_send_kernel, n_q // n_k),
        out_shape=jax.ShapeDtypeStruct((n_q, 3, tokens, head_dim), BF16),
        cost_estimate=pl.CostEstimate(flops=4 * q.size, bytes_accessed=12 * q.size, transcendentals=0),
        name='rope_send',
    )(q, k, v, cos, sin)


def local_kernel(scale, first_ref, q_ref, k_ref, v_ref, o_ref):
    block = pl.program_id(1)
    group, rows, _ = q_ref.shape
    span = WINDOW + rows
    start = pl.multiple_of(block * rows, rows)
    k = k_ref[0, pl.ds(start, span), :]
    v = v_ref[0, pl.ds(start, span), :]
    r = lax.broadcasted_iota(jnp.int32, (rows, span), 0)
    j = lax.broadcasted_iota(jnp.int32, (rows, span), 1)
    lowest = WINDOW - start - first_ref[0]
    allowed = (j <= r + WINDOW) & (j > r) & (j >= lowest)
    for h in range(group):
        s = lax.dot_general(q_ref[h], k, (((1,), (1,)), ((), ())), preferred_element_type=F32) * scale
        s = jnp.where(allowed, s, NEG)
        p = jnp.exp2(s - jnp.max(s, axis=1, keepdims=True))
        total = jnp.sum(p, axis=1, keepdims=True)
        out = jnp.dot(p.astype(BF16), v, preferred_element_type=F32) / total
        o_ref[h] = out.astype(BF16)


def local_attention(q, k_ext, v_ext, first):
    n_q, tokens, head_dim = q.shape
    n_k = k_ext.shape[0]
    group = n_q // n_k
    scale = math.log2(math.e) * head_dim ** -0.5
    flops = 4 * n_q * tokens * (WINDOW + Q_BLOCK) * head_dim
    return pl.pallas_call(
        functools.partial(local_kernel, scale),
        grid_spec=pltpu.PrefetchScalarGridSpec(
            num_scalar_prefetch=1,
            grid=(n_k, tokens // Q_BLOCK),
            in_specs=[
                pl.BlockSpec((group, Q_BLOCK, head_dim), lambda g, b, s: (g, b, 0)),
                pl.BlockSpec((1, k_ext.shape[1], head_dim), lambda g, b, s: (g, 0, 0)),
                pl.BlockSpec((1, k_ext.shape[1], head_dim), lambda g, b, s: (g, 0, 0)),
            ],
            out_specs=pl.BlockSpec((group, Q_BLOCK, head_dim), lambda g, b, s: (g, b, 0)),
        ),
        out_shape=jax.ShapeDtypeStruct((n_q, tokens, head_dim), BF16),
        cost_estimate=pl.CostEstimate(flops=2 * flops, bytes_accessed=4 * q.size, transcendentals=flops // (4 * head_dim)),
        name='local_attention',
    )(first, q, k_ext, v_ext)


def global_kernel(scale, offset, q_ref, k_ref, v_ref, o_ref, acc_ref, m_ref, l_ref):
    src = pl.program_id(0)
    q = q_ref[0, 0]
    rows = q.shape[0]

    def scores(k):
        return lax.dot_general(q, k, (((1,), (1,)), ((), ())), preferred_element_type=F32) * scale

    width = offset + rows
    s = scores(k_ref[src, :width])
    r = lax.broadcasted_iota(jnp.int32, (rows, width), 0)
    j = lax.broadcasted_iota(jnp.int32, (rows, width), 1)
    s = jnp.where(j <= r + offset, s, NEG)
    m = jnp.max(s, axis=1, keepdims=True)
    p = jnp.exp2(s - m)
    m_ref[...] = m
    l_ref[...] = jnp.sum(p, axis=1, keepdims=True)
    acc_ref[...] = jnp.dot(p.astype(BF16), v_ref[src, :width], preferred_element_type=F32)

    def step(i, _):
        s = scores(k_ref[i])
        m_old = m_ref[...]
        m_new = jnp.maximum(m_old, jnp.max(s, axis=1, keepdims=True))
        p = jnp.exp2(s - m_new)
        alpha = jnp.exp2(m_old - m_new)
        m_ref[...] = m_new
        l_ref[...] = l_ref[...] * alpha + jnp.sum(p, axis=1, keepdims=True)
        acc_ref[...] = acc_ref[...] * alpha + jnp.dot(p.astype(BF16), v_ref[i], preferred_element_type=F32)
        return 0

    lax.fori_loop(0, src, step, 0)
    o_ref[0] = (acc_ref[...] / l_ref[...]).astype(BF16)


def global_attention(received, k_all, v_all, offset):
    n_src, _, rows, head_dim = received.shape
    scale = math.log2(math.e) * head_dim ** -0.5
    total = k_all.shape[0] * k_all.shape[1]
    flops = 2 * n_src * rows * total * head_dim
    return pl.pallas_call(
        functools.partial(global_kernel, scale, offset),
        grid=(n_src,),
        in_specs=[
            pl.BlockSpec((1, 1, rows, head_dim), lambda s: (s, 0, 0, 0)),
            pl.BlockSpec(k_all.shape, lambda s: (0, 0, 0)),
            pl.BlockSpec(k_all.shape, lambda s: (0, 0, 0)),
        ],
        out_specs=pl.BlockSpec((1, rows, head_dim), lambda s: (s, 0, 0)),
        out_shape=jax.ShapeDtypeStruct((n_src, rows, head_dim), BF16),
        scratch_shapes=[pltpu.VMEM((rows, head_dim), F32), pltpu.VMEM((rows, 1), F32), pltpu.VMEM((rows, 1), F32)],
        cost_estimate=pl.CostEstimate(flops=2 * flops, bytes_accessed=8 * total * head_dim, transcendentals=flops // (4 * head_dim)),
        name='global_attention',
    )(received, k_all, v_all)


def normed(wide, gain):
    mean = jnp.mean(wide * wide, axis=1, keepdims=True)
    return wide * lax.rsqrt(mean + NORM_EPS) * gain


def joined(ref):
    return jnp.concatenate([ref[i] for i in range(ref.shape[0])], axis=1)


def norm_kernel(h_ref, gain_ref, u_ref):
    u_ref[...] = normed(joined(h_ref).astype(F32), gain_ref[...]).astype(BF16)


def norm_columns(h, gain):
    n, rows, columns = h.shape
    width, block = n * columns, 64
    return pl.pallas_call(
        norm_kernel,
        grid=(rows // block,),
        in_specs=[
            pl.BlockSpec((n, block, columns), lambda i: (0, i, 0)),
            pl.BlockSpec((1, width), lambda i: (0, 0)),
        ],
        out_specs=pl.BlockSpec((block, width), lambda i: (i, 0)),
        out_shape=jax.ShapeDtypeStruct((rows, width), BF16),
        cost_estimate=pl.CostEstimate(flops=6 * h.size, bytes_accessed=4 * h.size, transcendentals=rows),
        name='norm_columns',
    )(h, gain.reshape(1, width))


def finish_kernel(id_ref, h_ref, sum_ref, gain_ref, o_ref):
    del id_ref
    o_ref[...] = (joined(h_ref).astype(F32) + normed(sum_ref[...], gain_ref[...])).astype(BF16)


def finish(ids, h, total, gain):
    rows, width = total.shape
    n, _, columns = h.shape
    block = 32
    steps = rows // block
    return pl.pallas_call(
        finish_kernel,
        grid_spec=pltpu.PrefetchScalarGridSpec(
            num_scalar_prefetch=1,
            grid=(steps,),
            in_specs=[
                pl.BlockSpec((n, block, columns), lambda i, s: (0, s[0] * steps + i, 0)),
                pl.BlockSpec((block, width), lambda i, s: (i, 0)),
                pl.BlockSpec((1, width), lambda i, s: (0, 0)),
            ],
            out_specs=pl.BlockSpec((block, width), lambda i, s: (i, 0)),
        ),
        out_shape=jax.ShapeDtypeStruct((rows, width), BF16),
        cost_estimate=pl.CostEstimate(flops=8 * total.size, bytes_accessed=8 * total.size, transcendentals=rows),
        name='finish',
    )(ids, h, total, gain.reshape(1, width))


def output_kernel(id_ref, a_ref, w_ref, o_ref):
    del id_ref
    w = w_ref[...].reshape(w_ref.shape[0] * w_ref.shape[2], w_ref.shape[3])
    part = jnp.dot(joined(a_ref.at[0]), w, preferred_element_type=F32)

    @pl.when(pl.program_id(0) == 0)
    def _():
        o_ref[...] = part

    @pl.when(pl.program_id(0) > 0)
    def _():
        o_ref[...] += part


def output_projection(ids, attn, w):
    tp, heads, rows, head_dim = attn.shape
    columns = w.shape[3]
    return pl.pallas_call(
        output_kernel,
        grid_spec=pltpu.PrefetchScalarGridSpec(
            num_scalar_prefetch=1,
            grid=(tp,),
            in_specs=[
                pl.BlockSpec((1, heads, rows, head_dim), lambda k, s: (lax.rem(s[0] + tp - k, tp), 0, 0, 0)),
                pl.BlockSpec((heads, 1, head_dim, columns), lambda k, s: (0, k, 0, 0)),
            ],
            out_specs=pl.BlockSpec((rows, columns), lambda k, s: (0, 0)),
        ),
        out_shape=jax.ShapeDtypeStruct((rows, columns), F32),
        cost_estimate=pl.CostEstimate(flops=2 * attn.size * columns, bytes_accessed=2 * attn.size + 2 * w.size + 4 * rows * columns, transcendentals=0),
        name='output_projection',
    )(ids, attn, w)


def add_columns_kernel(width, id_ref, x_ref, o_ref, square_ref, gain_ref, h_ref):
    del id_ref
    inv_rms = lax.rsqrt(square_ref[...] / width + NORM_EPS)
    h_ref[...] = (x_ref[...].astype(F32) + o_ref[...] * inv_rms * gain_ref[...]).astype(BF16)


def add_columns(ids, x, first_row, o, squares, gain):
    rows, columns = o.shape
    width = x.shape[1]
    block = 128
    first_block = first_row // block
    return pl.pallas_call(
        functools.partial(add_columns_kernel, width),
        grid_spec=pltpu.PrefetchScalarGridSpec(
            num_scalar_prefetch=1,
            grid=(rows // block,),
            in_specs=[
                pl.BlockSpec((block, columns), lambda i, s: (first_block + i, s[0])),
                pl.BlockSpec((block, columns), lambda i, s: (i, 0)),
                pl.BlockSpec((block, 1), lambda i, s: (i, 0)),
                pl.BlockSpec((1, columns), lambda i, s: (0, s[0])),
            ],
            out_specs=pl.BlockSpec((block, columns), lambda i, s: (i, 0)),
        ),
        out_shape=jax.ShapeDtypeStruct((rows, columns), BF16),
        cost_estimate=pl.CostEstimate(flops=6 * o.size, bytes_accessed=8 * o.size, transcendentals=rows),
        name='add_columns',
    )(ids, x, o, squares.reshape(rows, 1), gain.reshape(1, width))


def dot(a, b):
    return jnp.dot(a, b, preferred_element_type=F32)


def solution(mesh):
    sp_size = mesh.shape['sp']
    tp_size = mesh.shape['tp']

    def device_fn(x_loc, pos_loc, gains, w_q, w_k, w_v, w_o, w_gate, w_up, w_down):
        seq, width = x_loc.shape
        heads_tp, head_dim = w_q.shape[2:]
        kv_tp = w_k.shape[2]
        share = sp_size // kv_tp
        sp_id = lax.axis_index('sp')
        tp_id = lax.axis_index('tp')
        rows = seq // CHUNKS

        def project(u, weights, l):
            return tuple(dot(u, w[l].reshape(width, -1)) for w in weights)

        def scatter(partial):
            return lax.psum_scatter(partial, 'tp', scatter_dimension=0, tiled=True)

        def gather(shard):
            return lax.all_gather(shard, 'tp', axis=0, tiled=True)

        ids = tp_id.astype(jnp.int32).reshape(1)
        columns = width // tp_size
        heads_dev = heads_tp // sp_size

        def spread(l):
            blocks = []
            for k in range(tp_size):
                target = lax.rem(tp_id + k, tp_size)
                block = lax.dynamic_slice(w_o, (l, sp_id * heads_dev, 0, target * columns), (1, heads_dev, head_dim, columns))[0]
                if k:
                    block = lax.ppermute(block, 'tp', [(i, (i + k) % tp_size) for i in range(tp_size)])
                blocks.append(block)
            return jnp.stack(blocks, axis=1)

        def collect(blocks):
            return lax.all_gather(blocks, 'sp', axis=0, tiled=True)

        def attn_tail(x, first_row, attn, w_columns, l, after):
            attn = lax.all_gather(attn, 'tp', axis=0)
            attn, _ = lax.optimization_barrier((attn, after[0]))
            o_sum = output_projection(ids, attn, w_columns)
            squares = lax.psum(jnp.sum(o_sum * o_sum, axis=1), 'tp')
            h1 = mine = add_columns(ids, x, first_row, o_sum, squares, gains[l, 1])
            h1 = lax.all_gather(h1, 'tp', axis=0)
            h1, _ = lax.optimization_barrier((h1, after[1]))
            u2 = norm_columns(h1, gains[l, 2])
            act = (jax.nn.silu(dot(u2, w_gate[l])) * dot(u2, w_up[l])).astype(BF16)
            m_part = dot(act, w_down[l])
            m_sum = scatter(m_part)
            out = finish(ids, h1, m_sum, gains[l, 3])
            out = gather(out)
            return out, (mine, m_part)

        u = rms_norm(x_loc, gains[0, 0]).astype(BF16)
        cos, sin = rope_tables(pos_loc, head_dim // 2, LOCAL_BASE)
        q, k, v = rope_local(*project(u, (w_q, w_k, w_v), 0), cos, sin)
        blocks = [spread(0), spread(1)]
        q, k, v, blocks = lax.optimization_barrier((q, k, v, blocks))
        tail = jnp.stack([k[:, seq - WINDOW:], v[:, seq - WINDOW:]])
        halo = lax.ppermute(tail, 'sp', [(i, i + 1) for i in range(sp_size - 1)])
        k_ext = jnp.concatenate([halo[0], k], axis=1)
        v_ext = jnp.concatenate([halo[1], v], axis=1)
        first = (sp_id * seq).astype(jnp.int32).reshape(1)
        w_columns = collect(blocks[0])
        attn = local_attention(q, k_ext, v_ext, first)
        tails = lax.all_gather(tail, 'sp', axis=0)[sp_size - 1]
        cache = lax.dynamic_index_in_dim(tails, sp_id // share, 1, keepdims=False)
        attn, cache, w_columns = lax.optimization_barrier((attn, cache, w_columns))
        later, attn = lax.optimization_barrier(((w_q, w_k, w_v), attn))

        cos, sin = rope_tables(pos_loc, head_dim // 2, GLOBAL_BASE)
        outs, received, after = [], [], (first, first)
        for c in range(CHUNKS):
            part = slice(c * rows, (c + 1) * rows)
            out, after = attn_tail(x_loc, c * rows, attn[:, part], w_columns, 0, after)
            if c:
                out, _ = lax.optimization_barrier((out, received[-1]))
            u = norm_columns(out[None], gains[1, 0])
            outgoing = rope_send(*project(u, later, 1), cos[part], sin[part])
            outs.append(out)
            received.append(lax.all_to_all(outgoing, 'sp', 0, 0, tiled=True))

        blocks, received[-1] = lax.optimization_barrier((blocks[1], received[-1]))
        w_columns = collect(blocks)
        k_all = jnp.concatenate([r[:, 1] for r in received], axis=1)
        v_all = jnp.concatenate([r[:, 2] for r in received], axis=1)
        finals = []
        for c in range(CHUNKS):
            attn = global_attention(received[c], k_all, v_all, c * rows)
            back = lax.all_to_all(attn, 'sp', 0, 0, tiled=True)
            if c == 0:
                back, w_columns = lax.optimization_barrier((back, w_columns))
            out, after = attn_tail(outs[c], 0, back, w_columns, 1, after)
            finals.append(out)
        hidden = jnp.concatenate(finals, axis=0)
        k_local, v_local = cache[0][:, None, :], cache[1][:, None, :]
        k_global = k_all.reshape(-1, 1, head_dim)
        v_global = v_all.reshape(-1, 1, head_dim)
        return hidden, k_local, v_local, k_global, v_global

    token_spec = P(('rep', 'sp'), None)
    cache_spec = P('rep', ('tp', 'sp'), None)
    in_specs = (token_spec, P(('rep', 'sp')), P(), P(None, None, 'tp', None), P(None, None, 'tp', None),
                P(None, None, 'tp', None), P(None, 'tp', None, None), P(None, None, 'tp'), P(None, None, 'tp'),
                P(None, 'tp', None))
    out_specs = (token_spec, cache_spec, cache_spec, cache_spec, cache_spec)
    return jax.shard_map(device_fn, mesh=mesh, in_specs=in_specs, out_specs=out_specs, check_vma=False)
```
